32 devices in a mesh: dp: 4 (over z), tensor: 8 (over y, x, core).
Axes of the slice: x: 2, y: 2, z: 4, core: 2. Of those that a mesh axis runs over, the one named last changes fastest.
Arguments:
- projected: bfloat16 [2, 4096, 4608], P(None, ('dp', 'tensor')), may hold values from -60 to 60
- out_grad: bfloat16 [2, 4096, 4608], P(None, ('dp', 'tensor')), may hold values from -20 to 20
- attention: bfloat16 [2, 4096, 4096], P(None, 'dp', 'tensor'), may hold values from -6 to 6
- w_out: bfloat16 [4096, 4608], P('tensor'), may hold values from -0.09375 to 0.09375
- gains: float32 [4608], replicated, may hold values from 0.5 to 1.5
- main_out: float32 [4096, 4608], P('tensor', 'dp'), may hold values from -6 to 6
- main_gains: float32 [4608], replicated, may hold values from -6 to 6
Outputs:
- attn_grad: bfloat16 [2, 4096, 4096], P(None, 'dp', 'tensor')
- new_main_out: float32 [4096, 4608], P('tensor', 'dp')
- new_main_gains: float32 [4608], replicated
The draws below stay inside these ranges and needn't reach their ends.
All inputs are finite; a program needn't handle non-finite values.
Results may differ from the reference program's by a relative error of at most 0.0049.
Values may be sent and summed in bfloat16 or wider, within the bound.
A program may use at most 128 MiB of HBM per device.

```python
import math
import jax
import jax.numpy as jnp
from jax import lax

D = 4608
HQ = 4096
MICRO = 2
ROWS = 4096


def spread_values(key, shape):
    first, second, third = jax.random.split(key, 3)
    base = jnp.clip(jax.random.normal(first, shape), -6.0, 6.0)
    columns = jnp.exp(jax.random.uniform(second, (shape[-1],), minval=math.log(0.3), maxval=math.log(3.0)))
    row_scale = jnp.exp(jax.random.uniform(third, shape[:-1] + (1,), minval=math.log(0.3), maxval=math.log(3.0)))
    return base * row_scale * columns


def rising_values(key, shape):
    position = jnp.arange(shape[1], dtype=jnp.float32) / shape[1]
    base = jnp.clip(jax.random.normal(key, shape), -6.0, 6.0)
    growth = jnp.exp(position * math.log(3.0))
    return base * growth[None, :, None]


def draw_projected(key, part):
    return spread_values(jax.random.fold_in(key, 22), (MICRO, ROWS, D)).astype(jnp.bfloat16)


def draw_out_grad(key, part):
    return rising_values(jax.random.fold_in(key, 33), (MICRO, ROWS, D)).astype(jnp.bfloat16)


def steps_of(stream_key, dims, cuts, low, high):
    def one(axis_at, shards_of):
        steps = jax.random.uniform(jax.random.fold_in(jax.random.fold_in(stream_key, 6), axis_at), (shards_of,), jnp.float32, low / len(cuts), high / len(cuts))
        return jnp.repeat(jnp.exp(steps), dims[axis_at] // shards_of).reshape((-1,) + (1,) * (len(dims) - axis_at - 1))

    loudness = one(*cuts[0])
    for cut in cuts[1:]:
        loudness = loudness * one(*cut)
    return loudness


def scatter_about(own_key, dims, spread, reach, cuts=(), held_as=jnp.bfloat16):
    result = jax.random.normal(own_key, dims, jnp.float32) * spread
    if len(cuts) > 0:
        result = steps_of(own_key, dims, cuts, -0.22, 0.18) * result
    return jnp.clip(result, min=-reach, max=reach).astype(held_as)


def setup_inputs(seed: int = 0) -> dict:
    keys = jax.random.split(jax.random.key(seed), 8)
    return {
        "projected": draw_projected(jax.random.fold_in(keys[7], 71), 0),
        "out_grad": draw_out_grad(jax.random.fold_in(keys[7], 71), 0),
        "attention": scatter_about(keys[2], (MICRO, ROWS, HQ), 1.0, 6.0, ((1, 4), (2, 8))),
        "w_out": scatter_about(keys[3], (HQ, D), HQ ** -0.5, 0.09375, ((0, 8),)),
        "gains": jnp.clip(1.0 + 0.1 * jax.random.normal(keys[4], (D,), jnp.float32), 0.5, 1.5),
        "main_out": scatter_about(keys[5], (HQ, D), 1.0, 6.0, ((0, 8), (1, 4)), jnp.float32),
        "main_gains": scatter_about(keys[6], (D,), 1.0, 6.0, (), jnp.float32),
    }


def normalized(values):
    inverse = lax.rsqrt(lax.optimization_barrier(jnp.mean(values * values, axis=-1, keepdims=True)) + 1e-06)
    return (values * inverse, inverse)

def norm_back(upstream, normed, inverse):
    return inverse * (upstream - normed * lax.optimization_barrier(jnp.mean(upstream * normed, axis=-1, keepdims=True)))

def reference(projected, out_grad, attention, w_out, gains, main_out, main_gains):
    factor = 1.0 / (MICRO * ROWS) ** 0.5
    sum_out = jnp.zeros((HQ, D), jnp.float32)
    sum_gain = jnp.zeros((D,), jnp.float32)
    attn_list = []
    for micro_step in range(MICRO):
        output_in = projected[micro_step].astype(jnp.float32)
        upstream = out_grad[micro_step].astype(jnp.float32)
        out_hat, out_inv = normalized(output_in)
        out_gain = lax.optimization_barrier(jnp.sum(upstream * out_hat, axis=0))
        out_back = norm_back(upstream * gains, out_hat, out_inv).astype(jnp.bfloat16)
        attn_list.append(jnp.dot(out_back, w_out.T, preferred_element_type=jnp.float32).astype(jnp.bfloat16))
        sum_out = sum_out + jnp.dot(attention[micro_step].T, out_back, preferred_element_type=jnp.float32)
        sum_gain = sum_gain + out_gain
    return (jnp.stack(attn_list), main_out + factor * sum_out, main_gains + factor * sum_gain)
```

```python
import functools
import math

import jax
import jax.numpy as jnp
from jax import lax
from jax.experimental import pallas as pl
from jax.experimental.pallas import tpu as pltpu
from jax.sharding import PartitionSpec as P

MESH = pl.DeviceIdType.MESH
LANES = 128
TILE = 16
VMEM_BYTES = 67043328


def flip(index, step):
    return index + step * (1 - 2 * (lax.div(index, step) % 2))


HOP = 3
LEAD = 3
GAP = 4


def kernel(
    dims,
    factor,
    proj_hbm, grad_hbm, att_hbm, w_hbm, main_hbm, gains_ref, main_gains_ref,
    attn_out, out_sum, gain_out,
    own_in, held, w_buf, att_in, att_t, acc, part, arrived,
    gains_row, scale, shift, gain_mine, gain_got,
    in_sem, w_sem, att_sem, main_sem,
    ag_send, ag_recv, pair_send, pair_recv, rs_send, rs_recv, gain_send, gain_recv,
):
    T, DP, D_true, micro, own, heads, wide, K, slots, ring, P, W = dims
    w = LANES
    R = micro * own
    L = (T // 2).bit_length() - 1
    C = T // 2
    O = DP - 1
    t_me = lax.axis_index("tensor")
    d_me = lax.axis_index("dp")
    c_me, chip_me = t_me % 2, lax.div(t_me, 2)
    d_width = wide // DP
    t_pair = flip(t_me, 1)
    chip_steps = [2 << bit for bit in range(L)]
    height = R // P
    span = C * R
    end = (K + O) * DP

    blocks = 8
    group = R // blocks

    def load(block):
        rows = pl.ds(block * group, group)
        return (
            pltpu.make_async_copy(proj_hbm.at[rows], own_in.at[0, rows], in_sem.at[block, 0]),
            pltpu.make_async_copy(grad_hbm.at[rows], own_in.at[1, rows], in_sem.at[block, 1]),
        )

    for block in range(blocks):
        for copy in load(block):
            copy.start()

    def att_load(t, slot):
        return [
            pltpu.make_async_copy(
                att_hbm.at[m, pl.ds(t * own, own)], att_in.at[slot, pl.ds(m * own, own)], att_sem.at[slot, m]
            )
            for m in range(micro)
        ]

    for t in range(slots):
        for copy in att_load(t, t):
            copy.start()
    main_in = pltpu.make_async_copy(main_hbm, out_sum, main_sem)

    def w_load(k, d):
        return pltpu.make_async_copy(
            w_hbm.at[:, pl.ds(pl.multiple_of(d * d_width + k * w, w), w)],
            w_buf.at[k, :, pl.ds(d * w, w)],
            w_sem,
        )

    barrier = pltpu.get_barrier_semaphore()
    partners = [("tensor", t_pair)] + [("tensor", flip(t_me, step)) for step in chip_steps]
    dp_steps = [1 << bit for bit in range(DP.bit_length() - 1)]
    partners += [("dp", flip(d_me, step)) for step in dp_steps]
    for name, where in partners:
        pl.semaphore_signal(barrier, inc=1, device_id={name: where}, device_id_type=MESH)

    @pl.when(d_me > 0)
    def _():
        pl.semaphore_signal(barrier, inc=1, device_id={"dp": d_me - 1}, device_id_type=MESH)

    @pl.when(d_me < DP - 1)
    def _():
        pl.semaphore_signal(barrier, inc=1, device_id={"dp": d_me + 1}, device_id_type=MESH)

    def place(n):
        s, j = lax.div(n, DP), lax.rem(n, DP)
        right = DP - 1 - d_me
        down = jnp.where(j < right, DP - 1 - j, j - right)
        up = jnp.where(j < d_me, j, DP - 1 - (j - d_me))
        d = jnp.where(j == DP - 1, d_me, jnp.where(2 * d_me < DP, down, up))
        lag = jnp.where(d > d_me, DP - 1 - d, jnp.where(d < d_me, d, O))
        k = s - lag
        good = jnp.logical_and(n >= 0, jnp.logical_and(k >= 0, k < K))
        return k, d, good

    def following(n):
        n = n + 1
        for _ in range(DP - 1):
            n = jnp.where(jnp.logical_or(place(n)[2], n >= end), n, n + 1)
        return n

    def turned(chip, p):
        return lax.div(chip, 1 << p) + (chip % (1 << p)) * (1 << (L - p))

    def home(parity, p, index):
        return pl.multiple_of(parity * span + (p * C + index) * height, LANES)

    gains_row[...] = gains_ref[...].reshape(1, wide)
    for block in range(blocks):
        for copy in load(block):
            copy.wait()

        def rows_step(i, carry, block=block):
            rows = pl.ds(pl.multiple_of(block * group + i * TILE, TILE), TILE)
            square = jnp.zeros((TILE, w), jnp.float32)
            cross = jnp.zeros((TILE, w), jnp.float32)
            for c0 in range(0, wide, w):
                v = own_in[0, rows, c0:c0 + w].astype(jnp.float32)
                g = own_in[1, rows, c0:c0 + w].astype(jnp.float32)
                square += v * v
                cross += (g * gains_row[:, c0:c0 + w]) * v
            r = lax.rsqrt(jnp.sum(square, axis=-1, keepdims=True) * (1.0 / D_true) + 1e-6)
            m = r * jnp.sum(cross, axis=-1, keepdims=True) * (1.0 / D_true)
            scale[rows, :] = jnp.broadcast_to(r, (TILE, w))
            shift[rows, :] = jnp.broadcast_to(r * m, (TILE, w))
            return carry

        lax.fori_loop(0, group // TILE, rows_step, 0)

    base = [home(c_me, p, turned(chip_me, p)) for p in range(P)]
    strip = 64

    def finish(n):
        k, d, good = place(n)

        @pl.when(good)
        def _():
            columns = pl.ds(pl.multiple_of(d * d_width + k * w, w), w)
            gain = gains_row[:, columns]
            total = jnp.zeros((8, w), jnp.float32)
            for i in range(0, R, strip):
                rows = pl.ds(i, strip)
                v = own_in[0, rows, columns].astype(jnp.float32)
                g = own_in[1, rows, columns].astype(jnp.float32)
                r = scale[rows, :]
                back = r * (g * gain - v * shift[rows, :])
                at = pl.ds(pl.multiple_of(base[i // height] + i % height, TILE), strip)
                held[k, d, at, :] = back.astype(jnp.bfloat16)
                gn = g * (v * r)
                for b in range(0, strip, 8):
                    total += gn[b:b + 8]
            gain_mine[0, :, columns] = jnp.sum(total, axis=0, keepdims=True)

    def grown(p, s, theirs):
        index = turned(chip_me, p)
        if theirs:
            index = flip(index, 1 << s)
        return pl.ds(home(c_me, p, lax.div(index, 1 << s) * (1 << s)), height << s)

    sent = [[grown(p, s, False) for p in range(P)] for s in range(L)]
    got = [[grown(p, s, True) for p in range(P)] for s in range(L)]

    def stage_copies(k, d, c, s, receive):
        copies = []
        for p in range(P):
            ref = held.at[k, d, (got if receive else sent)[s][p]]
            copies.append(pltpu.make_async_remote_copy(
                src_ref=ref, dst_ref=ref, send_sem=ag_send, recv_sem=ag_recv.at[c % W, s, p],
                device_id={"tensor": flip(t_me, chip_steps[(p + s) % L])}, device_id_type=MESH))
        return copies

    def half(parity):
        return pl.ds(pl.multiple_of(parity * span, span), span)

    def pair_copy(k, d, c, parity):
        ref = held.at[k, d, half(parity)]
        return pltpu.make_async_remote_copy(
            src_ref=ref, dst_ref=ref, send_sem=pair_send, recv_sem=pair_recv.at[c % W],
            device_id={"tensor": t_pair}, device_id_type=MESH)

    def advance(n, c, s, when=True):
        k, d, good = place(n)

        @pl.when(jnp.logical_and(good, when))
        def _():
            if s > 0:
                for copy in stage_copies(k, d, c, s - 1, True):
                    copy.wait_recv()
            if s < L:
                for copy in stage_copies(k, d, c, s, False):
                    copy.start()
            else:
                pair_copy(k, d, c, c_me).start()

    def start_w(k, carry):
        for d in range(DP):
            w_load(k, d).start()
        return carry

    def rs_copy(k, d, to_left):
        if to_left:
            slot = jnp.where(d_me - 1 == d, DP, d)
            peer = d_me - 1
        else:
            slot, peer = d, d_me + 1
        return pltpu.make_async_remote_copy(
            src_ref=arrived.at[k, d], dst_ref=arrived.at[k, slot], send_sem=rs_send,
            recv_sem=rs_recv.at[k, slot], device_id={"dp": peer}, device_id_type=MESH)

    def rs_arrival(k, slot):
        return pltpu.make_async_remote_copy(
            src_ref=arrived.at[k, slot], dst_ref=arrived.at[k, slot], send_sem=rs_send,
            recv_sem=rs_recv.at[k, slot], device_id={"dp": flip(d_me, 1)}, device_id_type=MESH)

    gain_steps = [("tensor", 1)] + [("tensor", s) for s in chip_steps] + [("dp", s) for s in dp_steps]
    S = len(gain_steps)

    def gain_copy(s):
        name, step = gain_steps[s]
        return pltpu.make_async_remote_copy(
            src_ref=gain_mine.at[s], dst_ref=gain_got.at[s], send_sem=gain_send.at[s], recv_sem=gain_recv.at[s],
            device_id={name: flip(t_me if name == "tensor" else d_me, step)}, device_id_type=MESH)

    look = [LEAD + GAP * (L - 1 - s) for s in range(L)]
    ahead = [jnp.int32(0)] * L

    def turn(t, carry):
        slot = t % slots
        for copy in att_load(t, slot):
            copy.wait()
        flat = att_in[slot].astype(jnp.float32).T.astype(jnp.bfloat16)
        for p in range(P):
            at = pl.ds(home(t % 2, p, turned(lax.div(t, 2), p)), height)
            att_t[:, at] = flat[:, p * height:(p + 1) * height]

        @pl.when(t + slots < T)
        def _():
            for copy in att_load(t + slots, slot):
                copy.start()
        return carry

    finish(ahead[0])
    waits = len(partners) + jnp.where(d_me > 0, 1, 0) + jnp.where(d_me < DP - 1, 1, 0)
    pl.semaphore_wait(barrier, waits)
    for i in range(look[0]):
        if i == look[0] - look[1] if L > 1 else i == look[0] - 1:
            lax.fori_loop(0, K, start_w, 0)
            main_in.start()
            lax.fori_loop(0, T, turn, 0)
        for s in reversed(range(L)):
            if i - look[0] + look[s] >= 0:
                if s == 0 and i > 0:
                    finish(ahead[0])
                advance(ahead[s], i - look[0] + look[s], s)
                ahead[s] = following(ahead[s])
    finish(ahead[0])
    main_in.wait()

    big = T * R // DP
    gain_from = (K * DP - look[0] + 1) // 2 + DP * (DP - 1) // 2 + 1

    def pass_on(n, to_left):
        k, d, good = place(n)
        mine = (d < d_me) if to_left else (d > d_me)
        has_arrival = (d_me < DP - 1) if to_left else (d_me > 0)

        @pl.when(jnp.logical_and(good, mine))
        def _():
            @pl.when(has_arrival)
            def _():
                rs_arrival(k, d).wait_recv()
                arrived[k, d] = (part[k % ring, d] + arrived[k, d].astype(jnp.float32)).astype(jnp.bfloat16)

            @pl.when(jnp.logical_not(has_arrival))
            def _():
                arrived[k, d] = part[k % ring, d].astype(jnp.bfloat16)

            rs_copy(k, d, to_left).start()

    def step(n, carry):
        done, late, todo, ahead = carry[0], carry[1], carry[2], list(carry[3:])
        k, d, good = place(n)
        advance(n, done, L)
        for s in reversed(range(L)):
            advance(ahead[s], done + look[s], s, good)
            ahead[s] = jnp.where(good, following(ahead[s]), ahead[s])

        first = jnp.logical_and(good, done == 0)
        ripe = jnp.logical_or(first, jnp.logical_and(late >= 0, jnp.logical_or(good, n - late >= 2)))
        chosen = jnp.where(ripe, jnp.where(first, n, late), -1)
        count = jnp.where(first, done, done - 1)

        @pl.when(ripe)
        def _():
            k, d, _ = place(chosen)
            pair_copy(k, d, count, 1 - c_me).wait_recv()
            part[k % ring, d] = jnp.dot(att_t[...], held[k, d], preferred_element_type=jnp.float32)

        pass_on(jnp.where(d_me == 0, chosen, n - HOP * d_me), False)
        pass_on(jnp.where(d_me == DP - 1, chosen, n - HOP * (DP - 1 - d_me)), True)

        for _ in range(2):
            @pl.when(good)
            def _(todo=todo):
                finish(todo)
            todo = jnp.where(good, following(todo), todo)
        c = lax.div(n - 2, DP) - O - 1
        j = lax.rem(n - 2, DP)

        @pl.when(jnp.logical_and(c >= 0, c < K))
        def _():
            @pl.when(j == 0)
            def _():
                @pl.when(c == 0)
                def _():
                    pltpu.make_async_copy(w_buf, w_buf, w_sem).wait()
            rows = pl.ds(pl.multiple_of(j * big, big), big)
            lhs = jnp.concatenate([held[c, e, rows, :] for e in range(DP)], axis=-1)
            value = lax.dot_general(
                lhs, w_buf[c], (((1,), (1,)), ((), ())), preferred_element_type=jnp.float32)

            @pl.when(c == 0)
            def _():
                acc[rows, :] = value

            @pl.when(jnp.logical_and(c > 0, c < K - 1))
            def _():
                acc[rows, :] += value

            @pl.when(c == K - 1)
            def _():
                last = (acc[rows, :] + value).astype(jnp.bfloat16)
                units, each = C * height // LANES, height // LANES
                for i in range(big // LANES):
                    at = j * (big // LANES) + i
                    parity, rest = lax.div(at, P * units), lax.rem(at, P * units)
                    p, rest = lax.div(rest, units), lax.rem(rest, units)
                    index, extra = lax.div(rest, each), lax.rem(rest, each)
                    chip = turned(index, 0)
                    for q in range(1, P):
                        chip = jnp.where(p == q, turned(index, L - q), chip)
                    row = p * height + extra * LANES
                    m, row = lax.div(row, own), lax.rem(row, own)
                    place_in = pl.ds(pl.multiple_of((chip * 2 + parity) * own + row, LANES), LANES)
                    attn_out[m, place_in, :] = last[i * LANES:(i + 1) * LANES]

        @pl.when(jnp.logical_and(jnp.logical_and(c >= 0, c < K), j == DP - 1))
        def _():
            at = pl.ds(pl.multiple_of(c * w, w), w)
            total = part[c % ring, d_me]
            out_sum[:, at] += factor * total

            @pl.when(d_me > 0)
            def _():
                rs_arrival(c, d_me).wait_recv()
                out_sum[:, at] += factor * arrived[c, d_me].astype(jnp.float32)

            @pl.when(d_me < DP - 1)
            def _():
                rs_arrival(c, DP).wait_recv()
                out_sum[:, at] += factor * arrived[c, DP].astype(jnp.float32)

        for s in range(S + 1):
            @pl.when(n == gain_from + 2 * s)
            def _(s=s):
                if s > 0:
                    gain_copy(s - 1).wait()
                    gain_mine[s] = gain_mine[s - 1] + gain_got[s - 1]
                if s < S:
                    gain_copy(s).start()
                else:
                    gain_out[...] = main_gains_ref[...] + factor * gain_mine[s].reshape(wide)

        late = jnp.where(
            jnp.logical_and(good, jnp.logical_not(first)), n, jnp.where(ripe, -1, late))
        return (done + jnp.where(good, 1, 0), late, todo, *ahead)

    total = max(end + DP + 2, gain_from + 2 * S + 1)
    lax.fori_loop(0, total, step, (jnp.int32(0), jnp.int32(-1), following(ahead[0]), *ahead))

    def sent_all(ref, sem):
        pltpu.make_async_remote_copy(
            src_ref=ref, dst_ref=ref, send_sem=sem, recv_sem=sem,
            device_id={"tensor": t_pair}, device_id_type=MESH).wait_send()

    sent_all(held.at[:, :, pl.ds(0, (C - 1) * R)], ag_send)
    sent_all(held.at[:, :, pl.ds(0, span)], pair_send)
    sent_all(arrived.at[:, pl.ds(0, DP - 1)], rs_send)


def emit(attn, total, gain, attn_hbm, total_hbm, gain_hbm, sem):
    copies = [
        pltpu.make_async_copy(attn, attn_hbm, sem.at[0]),
        pltpu.make_async_copy(total, total_hbm, sem.at[1]),
        pltpu.make_async_copy(gain, gain_hbm, sem.at[2]),
    ]
    for copy in copies:
        copy.start()
    for copy in copies:
        copy.wait()


def padded(values, parts, axis):
    size = values.shape[axis] // parts
    extra = -size % LANES
    if extra == 0:
        return values
    shape = values.shape
    split = values.reshape(shape[:axis] + (parts, size) + shape[axis + 1:])
    pads = [(0, 0)] * split.ndim
    pads[axis + 1] = (0, extra)
    return jnp.pad(split, pads).reshape(shape[:axis] + (parts * (size + extra),) + shape[axis + 1:])


def unpadded(values, parts, size, axis):
    have = values.shape[axis] // parts
    if have == size:
        return values
    shape = values.shape
    split = values.reshape(shape[:axis] + (parts, have) + shape[axis + 1:])
    split = lax.slice_in_dim(split, 0, size, axis=axis + 1)
    return split.reshape(shape[:axis] + (parts * size,) + shape[axis + 1:])


def per_device(projected, out_grad, attention, w_out, gains, main_out, main_gains):
    T, DP = lax.axis_size("tensor"), lax.axis_size("dp")
    micro, own, D = projected.shape
    heads = w_out.shape[0]
    piece = D // DP
    factor = 1.0 / math.sqrt(micro * own * DP * T)
    R = micro * own
    proj = padded(projected.reshape(R, D), DP, 1)
    grad = padded(out_grad.reshape(R, D), DP, 1)
    weight = padded(w_out, DP, 1)
    gain_row = padded(gains, DP, 0)
    main_gain_row = padded(main_gains, DP, 0)
    main = padded(main_out, 1, 1)
    wide = proj.shape[1]
    K = wide // DP // LANES
    C = T // 2
    L = C.bit_length() - 1
    S = 1 + L + DP.bit_length() - 1
    slots = 4
    ring = HOP * (DP - 1) // DP + 1
    P = min(L, R // LANES)
    P = P if R // LANES % P == 0 else 1
    W = 1 << (LEAD + GAP * (L - 1)).bit_length()
    dims = (T, DP, D, micro, own, heads, wide, K, slots, ring, P, W)
    DMA = pltpu.SemaphoreType.DMA
    hbm = pl.BlockSpec(memory_space=pltpu.HBM)
    vmem = pl.BlockSpec(memory_space=pltpu.VMEM)
    shapes = (
        ((micro, own * T, heads), jnp.bfloat16),
        ((heads, wide // DP), jnp.float32),
        ((wide,), jnp.float32),
    )
    kept = sum(math.prod(shape) * jnp.dtype(dtype).itemsize for shape, dtype in shapes) + (64 << 10)
    results = pl.pallas_call(
        functools.partial(kernel, dims, factor),
        out_shape=tuple(pltpu.VMEM(shape, dtype) for shape, dtype in shapes),
        in_specs=[hbm] * 5 + [vmem] * 2,
        out_specs=(vmem,) * 3,
        scratch_shapes=[
            pltpu.VMEM((2, R, wide), jnp.bfloat16),
            pltpu.VMEM((K, DP, T * R, LANES), jnp.bfloat16),
            pltpu.VMEM((K, heads, DP * LANES), jnp.bfloat16),
            pltpu.VMEM((slots, R, heads), jnp.bfloat16),
            pltpu.VMEM((heads, T * R), jnp.bfloat16),
            pltpu.VMEM((T * R, heads), jnp.float32),
            pltpu.VMEM((ring, DP, heads, LANES), jnp.float32),
            pltpu.VMEM((K, DP + 1, heads, LANES), jnp.bfloat16),
            pltpu.VMEM((1, wide), jnp.float32),
            pltpu.VMEM((R, LANES), jnp.float32),
            pltpu.VMEM((R, LANES), jnp.float32),
            pltpu.VMEM((S + 1, 1, wide), jnp.float32),
            pltpu.VMEM((S, 1, wide), jnp.float32),
            DMA((8, 2)), DMA, DMA((slots, micro)), DMA,
            DMA, DMA((W, L, P)), DMA, DMA((W,)), DMA, DMA((K, DP + 1)), DMA((S,)), DMA((S,)),
        ],
        compiler_params=pltpu.CompilerParams(
            collective_id=0, has_side_effects=True, vmem_limit_bytes=VMEM_BYTES - kept
        ),
    )(proj, grad, attention, weight, main, gain_row, main_gain_row)
    attn_grad, total, gain_total = pl.pallas_call(
        emit,
        out_shape=tuple(jax.ShapeDtypeStruct(shape, dtype) for shape, dtype in shapes),
        in_specs=[vmem] * 3,
        out_specs=(hbm,) * 3,
        scratch_shapes=[DMA((3,))],
        compiler_params=pltpu.CompilerParams(vmem_limit_bytes=1 << 20),
    )(*results)
    total = unpadded(total, 1, piece, 1)
    gain_total = unpadded(gain_total, DP, piece, 0).reshape(D)
    return (attn_grad, total, gain_total)


def solution(mesh):
    placed = (
        P(None, ("dp", "tensor"), None),
        P(None, ("dp", "tensor"), None),
        P(None, "dp", "tensor"),
        P("tensor", None),
        P(),
        P("tensor", "dp"),
        P(),
    )
    return jax.shard_map(
        per_device,
        mesh=mesh,
        in_specs=placed,
        out_specs=(P(None, "dp", "tensor"), P("tensor", "dp"), P()),
        check_vma=False,
    )
```

```python
import functools
import math

import jax
import jax.numpy as jnp
from jax import lax
from jax.experimental import pallas as pl
from jax.experimental.pallas import tpu as pltpu
from jax.sharding import PartitionSpec as P

MESH = pl.DeviceIdType.MESH
LANES = 128
TILE = 16
VMEM_BYTES = 67043328


def flip(index, step):
    return index + step * (1 - 2 * (lax.div(index, step) % 2))


HOP = 2
EXTRA = 4
QUEUE = 4
OWN_LAG = 2
EAGER = 6
LEAD = 3
GAP = 4


def kernel(
    dims,
    factor,
    proj_hbm, grad_hbm, att_hbm, w_hbm, main_hbm, gains_ref, main_gains_ref,
    attn_out, out_sum, gain_out,
    own_in, held, w_buf, att_in, att_t, acc, part, arrived,
    gains_row, scale, shift, gain_mine, gain_got, gain_all,
    in_sem, w_sem, att_sem, main_sem,
    ag_send, ag_recv, pair_send, pair_recv, rs_send, rs_recv, gain_send, gain_recv, share_send, share_recv,
):
    T, DP, D_true, micro, own, heads, wide, K, slots, ring, P, W = dims
    w = LANES
    R = micro * own
    L = (T // 2).bit_length() - 1
    C = T // 2
    O = min(OWN_LAG, DP - 1)
    A = max(O, DP - 2)
    t_me = lax.axis_index("tensor")
    d_me = lax.axis_index("dp")
    c_me, chip_me = t_me % 2, lax.div(t_me, 2)
    d_width = wide // DP
    t_pair = flip(t_me, 1)
    chip_steps = [2 << bit for bit in range(L)]
    height = R // P
    span = C * R
    end = (K + A) * DP

    blocks = 8
    group = R // blocks

    def load(block):
        rows = pl.ds(block * group, group)
        return (
            pltpu.make_async_copy(proj_hbm.at[rows], own_in.at[0, rows], in_sem.at[block, 0]),
            pltpu.make_async_copy(grad_hbm.at[rows], own_in.at[1, rows], in_sem.at[block, 1]),
        )

    for block in range(blocks):
        for copy in load(block):
            copy.start()

    def att_load(t, slot):
        return [
            pltpu.make_async_copy(
                att_hbm.at[m, pl.ds(t * own, own)], att_in.at[slot, pl.ds(m * own, own)], att_sem.at[slot, m]
            )
            for m in range(micro)
        ]

    for t in range(slots):
        for copy in att_load(t, t):
            copy.start()
    main_in = pltpu.make_async_copy(main_hbm, out_sum, main_sem)

    def w_load(k, d):
        return pltpu.make_async_copy(
            w_hbm.at[:, pl.ds(pl.multiple_of(d * d_width + k * w, w), w)],
            w_buf.at[k, :, pl.ds(d * w, w)],
            w_sem,
        )

    barrier = pltpu.get_barrier_semaphore()
    partners = [("tensor", t_pair)] + [("tensor", flip(t_me, step)) for step in chip_steps]
    others = [lax.rem(d_me + step, DP) for step in range(1, DP)]
    partners += [("dp", other) for other in others]
    for name, where in partners:
        pl.semaphore_signal(barrier, inc=1, device_id={name: where}, device_id_type=MESH)

    def place(n):
        s, j = lax.div(n, DP), lax.rem(n, DP)
        right = DP - 1 - d_me
        down = jnp.where(j < right, DP - 1 - j, j - right)
        up = jnp.where(j < d_me, j, DP - 1 - (j - d_me))
        d = jnp.where(j == DP - 1, d_me, jnp.where(2 * d_me < DP, down, up))
        lag = jnp.where(d > d_me, DP - 1 - d, jnp.where(d < d_me, d, O))
        k = s - lag
        good = jnp.logical_and(n >= 0, jnp.logical_and(k >= 0, k < K))
        return k, d, good

    def following(n):
        n = n + 1
        for _ in range(DP - 1):
            n = jnp.where(jnp.logical_or(place(n)[2], n >= end), n, n + 1)
        return n

    def turned(chip, p):
        return lax.div(chip, 1 << p) + (chip % (1 << p)) * (1 << (L - p))

    def home(parity, p, index):
        return pl.multiple_of(parity * span + (p * C + index) * height, LANES)

    gains_row[...] = gains_ref[...].reshape(1, wide)
    for block in range(blocks):
        for copy in load(block):
            copy.wait()

        def rows_step(i, carry, block=block):
            rows = pl.ds(pl.multiple_of(block * group + i * TILE, TILE), TILE)
            square = jnp.zeros((TILE, w), jnp.float32)
            cross = jnp.zeros((TILE, w), jnp.float32)
            for c0 in range(0, wide, w):
                v = own_in[0, rows, c0:c0 + w].astype(jnp.float32)
                g = own_in[1, rows, c0:c0 + w].astype(jnp.float32)
                square += v * v
                cross += (g * gains_row[:, c0:c0 + w]) * v
            r = lax.rsqrt(jnp.sum(square, axis=-1, keepdims=True) * (1.0 / D_true) + 1e-6)
            m = r * jnp.sum(cross, axis=-1, keepdims=True) * (1.0 / D_true)
            scale[rows, :] = jnp.broadcast_to(r, (TILE, w))
            shift[rows, :] = jnp.broadcast_to(r * m, (TILE, w))
            return carry

        lax.fori_loop(0, group // TILE, rows_step, 0)

    base = [home(c_me, p, turned(chip_me, p)) for p in range(P)]
    strip = 64

    def finish(n):
        k, d, good = place(n)

        @pl.when(good)
        def _():
            columns = pl.ds(pl.multiple_of(d * d_width + k * w, w), w)
            gain = gains_row[:, columns]
            total = jnp.zeros((8, w), jnp.float32)
            for i in range(0, R, strip):
                rows = pl.ds(i, strip)
                v = own_in[0, rows, columns].astype(jnp.float32)
                g = own_in[1, rows, columns].astype(jnp.float32)
                r = scale[rows, :]
                back = r * (g * gain - v * shift[rows, :])
                at = pl.ds(pl.multiple_of(base[i // height] + i % height, TILE), strip)
                held[k, d, at, :] = back.astype(jnp.bfloat16)
                gn = g * (v * r)
                for b in range(0, strip, 8):
                    total += gn[b:b + 8]
            gain_mine[0, :, columns] = jnp.sum(total, axis=0, keepdims=True)

    def grown(p, s, theirs):
        index = turned(chip_me, p)
        if theirs:
            index = flip(index, 1 << s)
        return pl.ds(home(c_me, p, lax.div(index, 1 << s) * (1 << s)), height << s)

    sent = [[grown(p, s, False) for p in range(P)] for s in range(L)]
    got = [[grown(p, s, True) for p in range(P)] for s in range(L)]

    def stage_copies(k, d, c, s, receive):
        copies = []
        for p in range(P):
            ref = held.at[k, d, (got if receive else sent)[s][p]]
            copies.append(pltpu.make_async_remote_copy(
                src_ref=ref, dst_ref=ref, send_sem=ag_send, recv_sem=ag_recv.at[c % W, s, p],
                device_id={"tensor": flip(t_me, chip_steps[(p + s) % L])}, device_id_type=MESH))
        return copies

    def half(parity):
        return pl.ds(pl.multiple_of(parity * span, span), span)

    def pair_copy(k, d, c, parity):
        ref = held.at[k, d, half(parity)]
        return pltpu.make_async_remote_copy(
            src_ref=ref, dst_ref=ref, send_sem=pair_send, recv_sem=pair_recv.at[c % W],
            device_id={"tensor": t_pair}, device_id_type=MESH)

    def advance(n, c, s, when=True):
        k, d, good = place(n)

        @pl.when(jnp.logical_and(good, when))
        def _():
            if s > 0:
                for copy in stage_copies(k, d, c, s - 1, True):
                    copy.wait_recv()
            if s < L:
                for copy in stage_copies(k, d, c, s, False):
                    copy.start()
            else:
                pair_copy(k, d, c, c_me).start()

    def start_w(k, carry):
        for d in range(DP):
            w_load(k, d).start()
        return carry

    def rs_copy(k, d, to_left, count):
        if to_left:
            slot = jnp.where(d_me - 1 == d, DP, d)
            peer = d_me - 1
        else:
            slot, peer = d, d_me + 1
        return pltpu.make_async_remote_copy(
            src_ref=arrived.at[k, d], dst_ref=arrived.at[k, slot], send_sem=rs_send.at[int(to_left), count % QUEUE],
            recv_sem=rs_recv.at[k, slot], device_id={"dp": peer}, device_id_type=MESH)

    def rs_arrival(k, slot):
        return pltpu.make_async_remote_copy(
            src_ref=arrived.at[k, slot], dst_ref=arrived.at[k, slot], send_sem=rs_send.at[0, 0],
            recv_sem=rs_recv.at[k, slot], device_id={"dp": flip(d_me, 1)}, device_id_type=MESH)

    gain_steps = [1] + chip_steps
    S = len(gain_steps)

    def gain_copy(s):
        return pltpu.make_async_remote_copy(
            src_ref=gain_mine.at[s], dst_ref=gain_got.at[s], send_sem=gain_send.at[s], recv_sem=gain_recv.at[s],
            device_id={"tensor": flip(t_me, gain_steps[s])}, device_id_type=MESH)

    def gain_share(step):
        return pltpu.make_async_remote_copy(
            src_ref=gain_mine.at[S], dst_ref=gain_all.at[d_me], send_sem=share_send.at[step],
            recv_sem=share_recv.at[d_me], device_id={"dp": others[step]}, device_id_type=MESH)

    def gain_shared(step):
        return pltpu.make_async_remote_copy(
            src_ref=gain_mine.at[S], dst_ref=gain_all.at[others[step]], send_sem=share_send.at[step],
            recv_sem=share_recv.at[others[step]], device_id={"dp": others[step]}, device_id_type=MESH)

    look = [LEAD + GAP * (L - 1 - s) for s in range(L)]
    ahead = [jnp.int32(0)] * L

    def turn(t, carry):
        slot = t % slots
        for copy in att_load(t, slot):
            copy.wait()
        flat = att_in[slot].astype(jnp.float32).T.astype(jnp.bfloat16)
        for p in range(P):
            at = pl.ds(home(t % 2, p, turned(lax.div(t, 2), p)), height)
            att_t[:, at] = flat[:, p * height:(p + 1) * height]

        @pl.when(t + slots < T)
        def _():
            for copy in att_load(t + slots, slot):
                copy.start()
        return carry

    finish(ahead[0])
    pl.semaphore_wait(barrier, len(partners))
    for i in range(look[0]):
        if i == look[0] - look[1] if L > 1 else i == look[0] - 1:
            lax.fori_loop(0, K, start_w, 0)
            main_in.start()
            lax.fori_loop(0, T, turn, 0)
        for s in reversed(range(L)):
            if i - look[0] + look[s] >= 0:
                if s == 0 and i > 0:
                    finish(ahead[0])
                advance(ahead[s], i - look[0] + look[s], s)
                ahead[s] = following(ahead[s])
    finish(ahead[0])
    main_in.wait()

    big = 2 * T * R // DP
    pairs = DP // 2
    gain_from = -(-(K * DP) // EAGER) + (A * DP) // 2 + 1

    def pass_on(n, to_left, count):
        k, d, good = place(n)
        mine = (d < d_me) if to_left else (d > d_me)
        has_arrival = (d_me < DP - 1) if to_left else (d_me > 0)
        go = jnp.logical_and(good, mine)

        @pl.when(go)
        def _():
            @pl.when(count >= QUEUE)
            def _():
                rs_copy(k, d, to_left, count).wait_send()

            @pl.when(has_arrival)
            def _():
                rs_arrival(k, d).wait_recv()
                arrived[k, d] = (part[k % ring, d] + arrived[k, d].astype(jnp.float32)).astype(jnp.bfloat16)

            @pl.when(jnp.logical_not(has_arrival))
            def _():
                arrived[k, d] = part[k % ring, d].astype(jnp.bfloat16)

            rs_copy(k, d, to_left, count).start()

        return count + jnp.where(go, 1, 0)

    def wait_of(hops):
        return jnp.where(hops == 0, 2, HOP * hops + EXTRA)

    def step(i, carry):
        done, todo, rights, lefts = carry[:4]
        ahead = list(carry[4:])

        def receive(n, done, ahead):
            good = place(n)[2]
            advance(n, done, L)
            moved = []
            for s in reversed(range(L)):
                advance(ahead[s], done + look[s], s, good)
                moved.insert(0, jnp.where(good, following(ahead[s]), ahead[s]))
            return done + jnp.where(good, 1, 0), moved

        before = done
        done, ahead = receive(2 * i, done, ahead)

        kx, dx, gx = place(2 * i - 2)
        ky, dy, gy = place(2 * i - 1)
        count = before - jnp.where(gx, 1, 0) - jnp.where(gy, 1, 0)

        @pl.when(jnp.logical_or(gx, gy))
        def _():
            tiles = ((kx, dx, gx, count), (ky, dy, gy, before - 1))
            for k, d, g, c in tiles:
                @pl.when(g)
                def _(k=k, d=d, c=c):
                    pair_copy(k, d, c, 1 - c_me).wait_recv()
            rhs = jnp.concatenate([
                held[jnp.where(gx, kx, ky), jnp.where(gx, dx, dy)],
                held[jnp.where(gy, ky, kx), jnp.where(gy, dy, dx)]], axis=-1)
            value = jnp.dot(att_t[...], rhs, preferred_element_type=jnp.float32)
            for e, (k, d, g, c) in enumerate(tiles):
                piece = value[:, e * w:(e + 1) * w]

                @pl.when(jnp.logical_and(g, d == d_me))
                def _(k=k, piece=piece):
                    at = pl.ds(pl.multiple_of(k * w, w), w)
                    out_sum[:, at] += factor * piece

                @pl.when(jnp.logical_and(g, d != d_me))
                def _(k=k, d=d, piece=piece):
                    part[k % ring, d] = piece

        done, ahead = receive(2 * i + 1, done, ahead)

        c = lax.div(i, pairs) - A - 1
        j = lax.rem(i, pairs)

        @pl.when(jnp.logical_and(c >= 0, c < K))
        def _():
            @pl.when(jnp.logical_and(c == 0, j == 0))
            def _():
                pltpu.make_async_copy(w_buf, w_buf, w_sem).wait()
            rows = pl.ds(pl.multiple_of(j * big, big), big)
            lhs = jnp.concatenate([held[c, e, rows, :] for e in range(DP)], axis=-1)
            value = lax.dot_general(
                lhs, w_buf[c], (((1,), (1,)), ((), ())), preferred_element_type=jnp.float32)

            @pl.when(c == 0)
            def _():
                acc[rows, :] = value

            @pl.when(jnp.logical_and(c > 0, c < K - 1))
            def _():
                acc[rows, :] += value

            @pl.when(c == K - 1)
            def _():
                last = (acc[rows, :] + value).astype(jnp.bfloat16)
                units, each = C * height // LANES, height // LANES
                for e in range(big // LANES):
                    at = j * (big // LANES) + e
                    parity, rest = lax.div(at, P * units), lax.rem(at, P * units)
                    p, rest = lax.div(rest, units), lax.rem(rest, units)
                    index, extra = lax.div(rest, each), lax.rem(rest, each)
                    chip = turned(index, 0)
                    for q in range(1, P):
                        chip = jnp.where(p == q, turned(index, L - q), chip)
                    row = p * height + extra * LANES
                    m, row = lax.div(row, own), lax.rem(row, own)
                    place_in = pl.ds(pl.multiple_of((chip * 2 + parity) * own + row, LANES), LANES)
                    attn_out[m, place_in, :] = last[e * LANES:(e + 1) * LANES]

        for e in range(2):
            rights = pass_on(2 * i + e - wait_of(d_me), False, rights)
            lefts = pass_on(2 * i + e - wait_of(DP - 1 - d_me), True, lefts)

        def more(x, todo):
            finish(todo)
            return following(todo)

        todo = lax.fori_loop(0, jnp.where(todo < end, EAGER, 0), more, todo)

        f = lax.div(i, pairs) - DP

        @pl.when(jnp.logical_and(jnp.logical_and(f >= 0, f < K), j == pairs - 1))
        def _():
            at = pl.ds(pl.multiple_of(f * w, w), w)

            @pl.when(d_me > 0)
            def _():
                rs_arrival(f, d_me).wait_recv()
                out_sum[:, at] += factor * arrived[f, d_me].astype(jnp.float32)

            @pl.when(d_me < DP - 1)
            def _():
                rs_arrival(f, DP).wait_recv()
                out_sum[:, at] += factor * arrived[f, DP].astype(jnp.float32)

        for s in range(S + 1):
            @pl.when(i == gain_from + s)
            def _(s=s):
                if s > 0:
                    gain_copy(s - 1).wait()
                    gain_mine[s] = gain_mine[s - 1] + gain_got[s - 1]
                if s < S:
                    gain_copy(s).start()
                else:
                    gain_all[d_me] = gain_mine[s]
                    for x in range(DP - 1):
                        gain_share(x).start()

        return (done, todo, rights, lefts, *ahead)

    total = max((K + A + 1) * pairs, (K + DP) * pairs, gain_from + S + 1)
    zero = jnp.int32(0)
    lax.fori_loop(0, total, step, (zero, following(ahead[0]), zero, zero, *ahead))

    def sent_all(ref, sem):
        pltpu.make_async_remote_copy(
            src_ref=ref, dst_ref=ref, send_sem=sem, recv_sem=sem,
            device_id={"tensor": t_pair}, device_id_type=MESH).wait_send()

    for x in range(DP - 1):
        gain_share(x).wait_send()
        gain_shared(x).wait_recv()
    gain_sum = gain_all[0]
    for x in range(1, DP):
        gain_sum = gain_sum + gain_all[x]
    gain_out[...] = main_gains_ref[...] + factor * gain_sum.reshape(wide)
    sent_all(held.at[:, :, pl.ds(0, (C - 1) * R)], ag_send)
    sent_all(held.at[:, :, pl.ds(0, span)], pair_send)
    for x in range(QUEUE):
        @pl.when(d_me < DP - 1)
        def _(x=x):
            sent_all(arrived.at[0, 0], rs_send.at[0, x])

        @pl.when(d_me > 0)
        def _(x=x):
            sent_all(arrived.at[0, 0], rs_send.at[1, x])


def emit(attn, total, gain, attn_hbm, total_hbm, gain_hbm, sem):
    copies = [
        pltpu.make_async_copy(attn, attn_hbm, sem.at[0]),
        pltpu.make_async_copy(total, total_hbm, sem.at[1]),
        pltpu.make_async_copy(gain, gain_hbm, sem.at[2]),
    ]
    for copy in copies:
        copy.start()
    for copy in copies:
        copy.wait()


def padded(values, parts, axis):
    size = values.shape[axis] // parts
    extra = -size % LANES
    if extra == 0:
        return values
    shape = values.shape
    split = values.reshape(shape[:axis] + (parts, size) + shape[axis + 1:])
    pads = [(0, 0)] * split.ndim
    pads[axis + 1] = (0, extra)
    return jnp.pad(split, pads).reshape(shape[:axis] + (parts * (size + extra),) + shape[axis + 1:])


def unpadded(values, parts, size, axis):
    have = values.shape[axis] // parts
    if have == size:
        return values
    shape = values.shape
    split = values.reshape(shape[:axis] + (parts, have) + shape[axis + 1:])
    split = lax.slice_in_dim(split, 0, size, axis=axis + 1)
    return split.reshape(shape[:axis] + (parts * size,) + shape[axis + 1:])


def per_device(projected, out_grad, attention, w_out, gains, main_out, main_gains):
    T, DP = lax.axis_size("tensor"), lax.axis_size("dp")
    micro, own, D = projected.shape
    heads = w_out.shape[0]
    piece = D // DP
    factor = 1.0 / math.sqrt(micro * own * DP * T)
    R = micro * own
    proj = padded(projected.reshape(R, D), DP, 1)
    grad = padded(out_grad.reshape(R, D), DP, 1)
    weight = padded(w_out, DP, 1)
    gain_row = padded(gains, DP, 0)
    main_gain_row = padded(main_gains, DP, 0)
    main = padded(main_out, 1, 1)
    wide = proj.shape[1]
    K = wide // DP // LANES
    C = T // 2
    L = C.bit_length() - 1
    S = 1 + L
    slots = 2
    ring = -(-(HOP * (DP - 2) + EXTRA) // DP)
    P = min(L, R // LANES)
    P = P if R // LANES % P == 0 else 1
    W = 1 << (LEAD + GAP * (L - 1)).bit_length()
    dims = (T, DP, D, micro, own, heads, wide, K, slots, ring, P, W)
    DMA = pltpu.SemaphoreType.DMA
    hbm = pl.BlockSpec(memory_space=pltpu.HBM)
    vmem = pl.BlockSpec(memory_space=pltpu.VMEM)
    shapes = (
        ((micro, own * T, heads), jnp.bfloat16),
        ((heads, wide // DP), jnp.float32),
        ((wide,), jnp.float32),
    )
    kept = sum(math.prod(shape) * jnp.dtype(dtype).itemsize for shape, dtype in shapes) + (64 << 10)
    results = pl.pallas_call(
        functools.partial(kernel, dims, factor),
        out_shape=tuple(pltpu.VMEM(shape, dtype) for shape, dtype in shapes),
        in_specs=[hbm] * 5 + [vmem] * 2,
        out_specs=(vmem,) * 3,
        scratch_shapes=[
            pltpu.VMEM((2, R, wide), jnp.bfloat16),
            pltpu.VMEM((K, DP, T * R, LANES), jnp.bfloat16),
            pltpu.VMEM((K, heads, DP * LANES), jnp.bfloat16),
            pltpu.VMEM((slots, R, heads), jnp.bfloat16),
            pltpu.VMEM((heads, T * R), jnp.bfloat16),
            pltpu.VMEM((T * R, heads), jnp.float32),
            pltpu.VMEM((ring, DP, heads, LANES), jnp.float32),
            pltpu.VMEM((K, DP + 1, heads, LANES), jnp.bfloat16),
            pltpu.VMEM((1, wide), jnp.float32),
            pltpu.VMEM((R, LANES), jnp.float32),
            pltpu.VMEM((R, LANES), jnp.float32),
            pltpu.VMEM((S + 1, 1, wide), jnp.float32),
            pltpu.VMEM((S, 1, wide), jnp.float32),
            pltpu.VMEM((DP, 1, wide), jnp.float32),
            DMA((8, 2)), DMA, DMA((slots, micro)), DMA,
            DMA, DMA((W, L, P)), DMA, DMA((W,)), DMA((2, QUEUE)), DMA((K, DP + 1)), DMA((S,)), DMA((S,)), DMA((DP - 1,)), DMA((DP,)),
        ],
        compiler_params=pltpu.CompilerParams(
            collective_id=0, has_side_effects=True, vmem_limit_bytes=VMEM_BYTES - kept
        ),
    )(proj, grad, attention, weight, main, gain_row, main_gain_row)
    attn_grad, total, gain_total = pl.pallas_call(
        emit,
        out_shape=tuple(jax.ShapeDtypeStruct(shape, dtype) for shape, dtype in shapes),
        in_specs=[vmem] * 3,
        out_specs=(hbm,) * 3,
        scratch_shapes=[DMA((3,))],
        compiler_params=pltpu.CompilerParams(vmem_limit_bytes=1 << 20),
    )(*results)
    total = unpadded(total, 1, piece, 1)
    gain_total = unpadded(gain_total, DP, piece, 0).reshape(D)
    return (attn_grad, total, gain_total)


def solution(mesh):
    placed = (
        P(None, ("dp", "tensor"), None),
        P(None, ("dp", "tensor"), None),
        P(None, "dp", "tensor"),
        P("tensor", None),
        P(),
        P("tensor", "dp"),
        P(),
    )
    return jax.shard_map(
        per_device,
        mesh=mesh,
        in_specs=placed,
        out_specs=(P(None, "dp", "tensor"), P("tensor", "dp"), P()),
        check_vma=False,
    )
```

```python
import functools
import math

import jax
import jax.numpy as jnp
from jax import lax
from jax.experimental import pallas as pl
from jax.experimental.pallas import tpu as pltpu
from jax.sharding import PartitionSpec as P

MESH = pl.DeviceIdType.MESH
LANES = 128
TILE = 16
VMEM_BYTES = 67043328


def flip(index, step):
    return index + step * (1 - 2 * (lax.div(index, step) % 2))


HOP = 2
EXTRA = 3
QUEUE = 4
OWN_LAG = 2
EAGER = 6
LEAD = 3
GAP = 4


def kernel(
    dims,
    factor,
    proj_hbm, grad_hbm, att_hbm, w_hbm, main_hbm, gains_ref, main_gains_ref,
    attn_out, out_sum, gain_out,
    own_in, held, w_buf, att_in, att_t, acc, part, arrived,
    gains_row, scale, shift, gain_mine, gain_got, gain_all,
    in_sem, w_sem, att_sem, main_sem,
    ag_send, ag_recv, pair_send, pair_recv, rs_send, rs_recv, gain_send, gain_recv, share_send, share_recv,
):
    T, DP, D_true, micro, own, heads, wide, K, slots, ring, P, W = dims
    w = LANES
    R = micro * own
    L = (T // 2).bit_length() - 1
    C = T // 2
    O = min(OWN_LAG, DP - 1)
    A = max(O, DP - 2)
    t_me = lax.axis_index("tensor")
    d_me = lax.axis_index("dp")
    c_me, chip_me = t_me % 2, lax.div(t_me, 2)
    d_width = wide // DP
    t_pair = flip(t_me, 1)
    chip_steps = [2 << bit for bit in range(L)]
    height = R // P
    span = C * R
    end = (K + A) * DP

    blocks = 8
    group = R // blocks

    def load(block):
        rows = pl.ds(block * group, group)
        return (
            pltpu.make_async_copy(proj_hbm.at[rows], own_in.at[0, rows], in_sem.at[block, 0]),
            pltpu.make_async_copy(grad_hbm.at[rows], own_in.at[1, rows], in_sem.at[block, 1]),
        )

    for block in range(blocks):
        for copy in load(block):
            copy.start()

    def att_load(t, slot):
        return [
            pltpu.make_async_copy(
                att_hbm.at[m, pl.ds(t * own, own)], att_in.at[slot, pl.ds(m * own, own)], att_sem.at[slot, m]
            )
            for m in range(micro)
        ]

    for t in range(slots):
        for copy in att_load(t, t):
            copy.start()
    main_in = pltpu.make_async_copy(main_hbm, out_sum, main_sem)

    def w_load(k, d):
        return pltpu.make_async_copy(
            w_hbm.at[:, pl.ds(pl.multiple_of(d * d_width + k * w, w), w)],
            w_buf.at[k, :, pl.ds(d * w, w)],
            w_sem,
        )

    barrier = pltpu.get_barrier_semaphore()
    partners = [("tensor", t_pair)] + [("tensor", flip(t_me, step)) for step in chip_steps]
    others = [lax.rem(d_me + step, DP) for step in range(1, DP)]
    partners += [("dp", other) for other in others]
    for name, where in partners:
        pl.semaphore_signal(barrier, inc=1, device_id={name: where}, device_id_type=MESH)

    def place(n):
        s, j = lax.div(n, DP), lax.rem(n, DP)
        right = DP - 1 - d_me
        down = jnp.where(j < right, DP - 1 - j, j - right)
        up = jnp.where(j < d_me, j, DP - 1 - (j - d_me))
        d = jnp.where(j == DP - 1, d_me, jnp.where(2 * d_me < DP, down, up))
        lag = jnp.where(d > d_me, DP - 1 - d, jnp.where(d < d_me, d, O))
        k = s - lag
        good = jnp.logical_and(n >= 0, jnp.logical_and(k >= 0, k < K))
        return k, d, good

    def following(n):
        n = n + 1
        for _ in range(DP - 1):
            n = jnp.where(jnp.logical_or(place(n)[2], n >= end), n, n + 1)
        return n

    def turned(chip, p):
        return lax.div(chip, 1 << p) + (chip % (1 << p)) * (1 << (L - p))

    def home(parity, p, index):
        return pl.multiple_of(parity * span + (p * C + index) * height, LANES)

    gains_row[...] = gains_ref[...].reshape(1, wide)
    for block in range(blocks):
        for copy in load(block):
            copy.wait()

        def rows_step(i, carry, block=block):
            rows = pl.ds(pl.multiple_of(block * group + i * TILE, TILE), TILE)
            square = jnp.zeros((TILE, w), jnp.float32)
            cross = jnp.zeros((TILE, w), jnp.float32)
            for c0 in range(0, wide, w):
                v = own_in[0, rows, c0:c0 + w].astype(jnp.float32)
                g = own_in[1, rows, c0:c0 + w].astype(jnp.float32)
                square += v * v
                cross += (g * gains_row[:, c0:c0 + w]) * v
            r = lax.rsqrt(jnp.sum(square, axis=-1, keepdims=True) * (1.0 / D_true) + 1e-6)
            m = r * jnp.sum(cross, axis=-1, keepdims=True) * (1.0 / D_true)
            scale[rows, :] = jnp.broadcast_to(r, (TILE, w))
            shift[rows, :] = jnp.broadcast_to(r * m, (TILE, w))
            return carry

        lax.fori_loop(0, group // TILE, rows_step, 0)

    base = [home(c_me, p, turned(chip_me, p)) for p in range(P)]
    strip = 64

    def finish(n):
        k, d, good = place(n)

        @pl.when(good)
        def _():
            columns = pl.ds(pl.multiple_of(d * d_width + k * w, w), w)
            gain = gains_row[:, columns]
            total = jnp.zeros((8, w), jnp.float32)
            for i in range(0, R, strip):
                rows = pl.ds(i, strip)
                v = own_in[0, rows, columns].astype(jnp.float32)
                g = own_in[1, rows, columns].astype(jnp.float32)
                r = scale[rows, :]
                back = r * (g * gain - v * shift[rows, :])
                at = pl.ds(pl.multiple_of(base[i // height] + i % height, TILE), strip)
                held[k, d, at, :] = back.astype(jnp.bfloat16)
                gn = g * (v * r)
                for b in range(0, strip, 8):
                    total += gn[b:b + 8]
            gain_mine[0, :, columns] = jnp.sum(total, axis=0, keepdims=True)

    def grown(p, s, theirs):
        index = turned(chip_me, p)
        if theirs:
            index = flip(index, 1 << s)
        return pl.ds(home(c_me, p, lax.div(index, 1 << s) * (1 << s)), height << s)

    sent = [[grown(p, s, False) for p in range(P)] for s in range(L)]
    got = [[grown(p, s, True) for p in range(P)] for s in range(L)]

    def stage_copies(k, d, c, s, receive):
        copies = []
        for p in range(P):
            ref = held.at[k, d, (got if receive else sent)[s][p]]
            copies.append(pltpu.make_async_remote_copy(
                src_ref=ref, dst_ref=ref, send_sem=ag_send, recv_sem=ag_recv.at[c % W, s, p],
                device_id={"tensor": flip(t_me, chip_steps[(p + s) % L])}, device_id_type=MESH))
        return copies

    def half(parity):
        return pl.ds(pl.multiple_of(parity * span, span), span)

    def pair_copy(k, d, c, parity):
        ref = held.at[k, d, half(parity)]
        return pltpu.make_async_remote_copy(
            src_ref=ref, dst_ref=ref, send_sem=pair_send, recv_sem=pair_recv.at[c % W],
            device_id={"tensor": t_pair}, device_id_type=MESH)

    def advance(n, c, s):
        k, d, good = place(n)

        @pl.when(good)
        def _():
            if s > 0:
                for copy in stage_copies(k, d, c, s - 1, True):
                    copy.wait_recv()
            if s < L:
                for copy in stage_copies(k, d, c, s, False):
                    copy.start()
            else:
                pair_copy(k, d, c, c_me).start()

    def start_w(k, carry):
        for d in range(DP):
            w_load(k, d).start()
        return carry

    def rs_copy(k, d, to_left, count):
        if to_left:
            slot = jnp.where(d_me - 1 == d, DP, d)
            peer = d_me - 1
        else:
            slot, peer = d, d_me + 1
        return pltpu.make_async_remote_copy(
            src_ref=arrived.at[k, d], dst_ref=arrived.at[k, slot], send_sem=rs_send.at[int(to_left), count % QUEUE],
            recv_sem=rs_recv.at[k, slot], device_id={"dp": peer}, device_id_type=MESH)

    def rs_arrival(k, slot):
        return pltpu.make_async_remote_copy(
            src_ref=arrived.at[k, slot], dst_ref=arrived.at[k, slot], send_sem=rs_send.at[0, 0],
            recv_sem=rs_recv.at[k, slot], device_id={"dp": flip(d_me, 1)}, device_id_type=MESH)

    gain_steps = [1] + chip_steps
    S = len(gain_steps)

    def gain_copy(s):
        return pltpu.make_async_remote_copy(
            src_ref=gain_mine.at[s], dst_ref=gain_got.at[s], send_sem=gain_send.at[s], recv_sem=gain_recv.at[s],
            device_id={"tensor": flip(t_me, gain_steps[s])}, device_id_type=MESH)

    def gain_share(step):
        return pltpu.make_async_remote_copy(
            src_ref=gain_mine.at[S], dst_ref=gain_all.at[d_me], send_sem=share_send.at[step],
            recv_sem=share_recv.at[d_me], device_id={"dp": others[step]}, device_id_type=MESH)

    def gain_shared(step):
        return pltpu.make_async_remote_copy(
            src_ref=gain_mine.at[S], dst_ref=gain_all.at[others[step]], send_sem=share_send.at[step],
            recv_sem=share_recv.at[others[step]], device_id={"dp": others[step]}, device_id_type=MESH)

    look = [LEAD + GAP * (L - 1 - s) for s in range(L)]
    ahead = [jnp.int32(0)] * L

    def turn(t, carry):
        slot = t % slots
        for copy in att_load(t, slot):
            copy.wait()
        flat = att_in[slot].astype(jnp.float32).T.astype(jnp.bfloat16)
        for p in range(P):
            at = pl.ds(home(t % 2, p, turned(lax.div(t, 2), p)), height)
            att_t[:, at] = flat[:, p * height:(p + 1) * height]

        @pl.when(t + slots < T)
        def _():
            for copy in att_load(t + slots, slot):
                copy.start()
        return carry

    finish(ahead[0])
    pl.semaphore_wait(barrier, len(partners))
    for i in range(look[0]):
        if i == look[0] - look[1] if L > 1 else i == look[0] - 1:
            lax.fori_loop(0, K, start_w, 0)
            main_in.start()
            lax.fori_loop(0, T // 2, turn, 0)
        for s in reversed(range(L)):
            if i - look[0] + look[s] >= 0:
                if s == 0 and i > 0:
                    finish(ahead[0])
                advance(ahead[s], i - look[0] + look[s], s)
                ahead[s] = following(ahead[s])
    lax.fori_loop(T // 2, T, turn, 0)
    finish(ahead[0])
    main_in.wait()

    big = 2 * T * R // DP
    pairs = DP // 2
    gain_from = -(-(K * DP) // EAGER) + (A * DP) // 2 + 1

    def pass_on(n, to_left, count):
        k, d, good = place(n)
        mine = (d < d_me) if to_left else (d > d_me)
        has_arrival = (d_me < DP - 1) if to_left else (d_me > 0)
        go = jnp.logical_and(good, mine)

        @pl.when(go)
        def _():
            @pl.when(count >= QUEUE)
            def _():
                rs_copy(k, d, to_left, count).wait_send()

            @pl.when(has_arrival)
            def _():
                rs_arrival(k, d).wait_recv()
                arrived[k, d] = (part[k % ring, d] + arrived[k, d].astype(jnp.float32)).astype(jnp.bfloat16)

            @pl.when(jnp.logical_not(has_arrival))
            def _():
                arrived[k, d] = part[k % ring, d].astype(jnp.bfloat16)

            rs_copy(k, d, to_left, count).start()

        return count + jnp.where(go, 1, 0)

    def wait_of(hops):
        return jnp.where(hops == 0, 2, HOP * hops + EXTRA)

    def step(i, carry):
        done, todo, rights, lefts = carry[:4]
        ahead = carry[4:]

        def receive(n, done, ahead):
            good = place(n)[2]
            advance(n, done, L)
            times = jnp.where(good, 1, 0)

            def issue(x, ahead):
                moved = []
                for s in reversed(range(L)):
                    spot, index = ahead[2 * s], ahead[2 * s + 1]
                    advance(spot, index, s)
                    moved = [following(spot), index + 1] + moved
                return tuple(moved)

            return done + times, lax.fori_loop(0, times, issue, tuple(ahead))

        before = done
        done, ahead = receive(2 * i, done, ahead)

        kx, dx, gx = place(2 * i - 2)
        ky, dy, gy = place(2 * i - 1)
        count = before - jnp.where(gx, 1, 0) - jnp.where(gy, 1, 0)

        @pl.when(jnp.logical_or(gx, gy))
        def _():
            tiles = ((kx, dx, gx, count), (ky, dy, gy, before - 1))
            for k, d, g, c in tiles:
                @pl.when(g)
                def _(k=k, d=d, c=c):
                    pair_copy(k, d, c, 1 - c_me).wait_recv()
            rhs = jnp.concatenate([
                held[jnp.where(gx, kx, ky), jnp.where(gx, dx, dy)],
                held[jnp.where(gy, ky, kx), jnp.where(gy, dy, dx)]], axis=-1)
            value = jnp.dot(att_t[...], rhs, preferred_element_type=jnp.float32)
            for e, (k, d, g, c) in enumerate(tiles):
                piece = value[:, e * w:(e + 1) * w]

                @pl.when(jnp.logical_and(g, d == d_me))
                def _(k=k, piece=piece):
                    at = pl.ds(pl.multiple_of(k * w, w), w)
                    out_sum[:, at] += factor * piece

                @pl.when(jnp.logical_and(g, d != d_me))
                def _(k=k, d=d, piece=piece):
                    part[k % ring, d] = piece

        for e in range(2):
            rights = pass_on(2 * i + e - wait_of(d_me), False, rights)
            lefts = pass_on(2 * i + e - wait_of(DP - 1 - d_me), True, lefts)

        done, ahead = receive(2 * i + 1, done, ahead)

        c = lax.div(i, pairs) - A - 1
        j = lax.rem(i, pairs)

        @pl.when(jnp.logical_and(c >= 0, c < K))
        def _():
            @pl.when(jnp.logical_and(c == 0, j == 0))
            def _():
                pltpu.make_async_copy(w_buf, w_buf, w_sem).wait()
            rows = pl.ds(pl.multiple_of(j * big, big), big)
            lhs = jnp.concatenate([held[c, e, rows, :] for e in range(DP)], axis=-1)
            value = lax.dot_general(
                lhs, w_buf[c], (((1,), (1,)), ((), ())), preferred_element_type=jnp.float32)

            @pl.when(c == 0)
            def _():
                acc[rows, :] = value

            @pl.when(jnp.logical_and(c > 0, c < K - 1))
            def _():
                acc[rows, :] += value

            @pl.when(c == K - 1)
            def _():
                last = (acc[rows, :] + value).astype(jnp.bfloat16)
                units, each = C * height // LANES, height // LANES
                for e in range(big // LANES):
                    at = j * (big // LANES) + e
                    parity, rest = lax.div(at, P * units), lax.rem(at, P * units)
                    p, rest = lax.div(rest, units), lax.rem(rest, units)
                    index, extra = lax.div(rest, each), lax.rem(rest, each)
                    chip = turned(index, 0)
                    for q in range(1, P):
                        chip = jnp.where(p == q, turned(index, L - q), chip)
                    row = p * height + extra * LANES
                    m, row = lax.div(row, own), lax.rem(row, own)
                    place_in = pl.ds(pl.multiple_of((chip * 2 + parity) * own + row, LANES), LANES)
                    attn_out[m, place_in, :] = last[e * LANES:(e + 1) * LANES]

        def more(x, todo):
            finish(todo)
            return following(todo)

        todo = lax.fori_loop(0, jnp.where(todo < end, EAGER, 0), more, todo)

        f = lax.div(i, pairs) - DP

        @pl.when(jnp.logical_and(jnp.logical_and(f >= 0, f < K), j == pairs - 1))
        def _():
            at = pl.ds(pl.multiple_of(f * w, w), w)

            @pl.when(d_me > 0)
            def _():
                rs_arrival(f, d_me).wait_recv()
                out_sum[:, at] += factor * arrived[f, d_me].astype(jnp.float32)

            @pl.when(d_me < DP - 1)
            def _():
                rs_arrival(f, DP).wait_recv()
                out_sum[:, at] += factor * arrived[f, DP].astype(jnp.float32)

        for s in range(S + 1):
            @pl.when(i == gain_from + s)
            def _(s=s):
                if s > 0:
                    gain_copy(s - 1).wait()
                    gain_mine[s] = gain_mine[s - 1] + gain_got[s - 1]
                if s < S:
                    gain_copy(s).start()
                else:
                    gain_all[d_me] = gain_mine[s]
                    for x in range(DP - 1):
                        gain_share(x).start()

        return (done, todo, rights, lefts, *ahead)

    total = max((K + A + 1) * pairs, (K + DP) * pairs, gain_from + S + 1)
    zero = jnp.int32(0)
    queue = [value for s in range(L) for value in (ahead[s], zero + look[s])]
    lax.fori_loop(0, total, step, (zero, following(ahead[0]), zero, zero, *queue))

    def sent_all(ref, sem):
        pltpu.make_async_remote_copy(
            src_ref=ref, dst_ref=ref, send_sem=sem, recv_sem=sem,
            device_id={"tensor": t_pair}, device_id_type=MESH).wait_send()

    for x in range(DP - 1):
        gain_share(x).wait_send()
        gain_shared(x).wait_recv()
    gain_sum = gain_all[0]
    for x in range(1, DP):
        gain_sum = gain_sum + gain_all[x]
    gain_out[...] = main_gains_ref[...] + factor * gain_sum.reshape(wide)
    sent_all(held.at[:, :, pl.ds(0, (C - 1) * R)], ag_send)
    sent_all(held.at[:, :, pl.ds(0, span)], pair_send)
    for x in range(QUEUE):
        @pl.when(d_me < DP - 1)
        def _(x=x):
            sent_all(arrived.at[0, 0], rs_send.at[0, x])

        @pl.when(d_me > 0)
        def _(x=x):
            sent_all(arrived.at[0, 0], rs_send.at[1, x])


def emit(attn, total, gain, attn_hbm, total_hbm, gain_hbm, sem):
    copies = [
        pltpu.make_async_copy(attn, attn_hbm, sem.at[0]),
        pltpu.make_async_copy(total, total_hbm, sem.at[1]),
        pltpu.make_async_copy(gain, gain_hbm, sem.at[2]),
    ]
    for copy in copies:
        copy.start()
    for copy in copies:
        copy.wait()


def padded(values, parts, axis):
    size = values.shape[axis] // parts
    extra = -size % LANES
    if extra == 0:
        return values
    shape = values.shape
    split = values.reshape(shape[:axis] + (parts, size) + shape[axis + 1:])
    pads = [(0, 0)] * split.ndim
    pads[axis + 1] = (0, extra)
    return jnp.pad(split, pads).reshape(shape[:axis] + (parts * (size + extra),) + shape[axis + 1:])


def unpadded(values, parts, size, axis):
    have = values.shape[axis] // parts
    if have == size:
        return values
    shape = values.shape
    split = values.reshape(shape[:axis] + (parts, have) + shape[axis + 1:])
    split = lax.slice_in_dim(split, 0, size, axis=axis + 1)
    return split.reshape(shape[:axis] + (parts * size,) + shape[axis + 1:])


def per_device(projected, out_grad, attention, w_out, gains, main_out, main_gains):
    T, DP = lax.axis_size("tensor"), lax.axis_size("dp")
    micro, own, D = projected.shape
    heads = w_out.shape[0]
    piece = D // DP
    factor = 1.0 / math.sqrt(micro * own * DP * T)
    R = micro * own
    proj = padded(projected.reshape(R, D), DP, 1)
    grad = padded(out_grad.reshape(R, D), DP, 1)
    weight = padded(w_out, DP, 1)
    gain_row = padded(gains, DP, 0)
    main_gain_row = padded(main_gains, DP, 0)
    main = padded(main_out, 1, 1)
    wide = proj.shape[1]
    K = wide // DP // LANES
    C = T // 2
    L = C.bit_length() - 1
    S = 1 + L
    slots = 4
    ring = -(-(HOP * (DP - 2) + EXTRA) // DP)
    P = min(L, R // LANES)
    P = P if R // LANES % P == 0 else 1
    W = LEAD + GAP * (L - 1) + 1
    dims = (T, DP, D, micro, own, heads, wide, K, slots, ring, P, W)
    DMA = pltpu.SemaphoreType.DMA
    hbm = pl.BlockSpec(memory_space=pltpu.HBM)
    vmem = pl.BlockSpec(memory_space=pltpu.VMEM)
    shapes = (
        ((micro, own * T, heads), jnp.bfloat16),
        ((heads, wide // DP), jnp.float32),
        ((wide,), jnp.float32),
    )
    kept = sum(math.prod(shape) * jnp.dtype(dtype).itemsize for shape, dtype in shapes) + (64 << 10)
    results = pl.pallas_call(
        functools.partial(kernel, dims, factor),
        out_shape=tuple(pltpu.VMEM(shape, dtype) for shape, dtype in shapes),
        in_specs=[hbm] * 5 + [vmem] * 2,
        out_specs=(vmem,) * 3,
        scratch_shapes=[
            pltpu.VMEM((2, R, wide), jnp.bfloat16),
            pltpu.VMEM((K, DP, T * R, LANES), jnp.bfloat16),
            pltpu.VMEM((K, heads, DP * LANES), jnp.bfloat16),
            pltpu.VMEM((slots, R, heads), jnp.bfloat16),
            pltpu.VMEM((heads, T * R), jnp.bfloat16),
            pltpu.VMEM((T * R, heads), jnp.float32),
            pltpu.VMEM((ring, DP, heads, LANES), jnp.float32),
            pltpu.VMEM((K, DP + 1, heads, LANES), jnp.bfloat16),
            pltpu.VMEM((1, wide), jnp.float32),
            pltpu.VMEM((R, LANES), jnp.float32),
            pltpu.VMEM((R, LANES), jnp.float32),
            pltpu.VMEM((S + 1, 1, wide), jnp.float32),
            pltpu.VMEM((S, 1, wide), jnp.float32),
            pltpu.VMEM((DP, 1, wide), jnp.float32),
            DMA((8, 2)), DMA, DMA((slots, micro)), DMA,
            DMA, DMA((W, L, P)), DMA, DMA((W,)), DMA((2, QUEUE)), DMA((K, DP + 1)), DMA((S,)), DMA((S,)), DMA((DP - 1,)), DMA((DP,)),
        ],
        compiler_params=pltpu.CompilerParams(
            collective_id=0, has_side_effects=True, vmem_limit_bytes=VMEM_BYTES - kept
        ),
    )(proj, grad, attention, weight, main, gain_row, main_gain_row)
    attn_grad, total, gain_total = pl.pallas_call(
        emit,
        out_shape=tuple(jax.ShapeDtypeStruct(shape, dtype) for shape, dtype in shapes),
        in_specs=[vmem] * 3,
        out_specs=(hbm,) * 3,
        scratch_shapes=[DMA((3,))],
        compiler_params=pltpu.CompilerParams(vmem_limit_bytes=1 << 20),
    )(*results)
    total = unpadded(total, 1, piece, 1)
    gain_total = unpadded(gain_total, DP, piece, 0).reshape(D)
    return (attn_grad, total, gain_total)


def solution(mesh):
    placed = (
        P(None, ("dp", "tensor"), None),
        P(None, ("dp", "tensor"), None),
        P(None, "dp", "tensor"),
        P("tensor", None),
        P(),
        P("tensor", "dp"),
        P(),
    )
    return jax.shard_map(
        per_device,
        mesh=mesh,
        in_specs=placed,
        out_specs=(P(None, "dp", "tensor"), P("tensor", "dp"), P()),
        check_vma=False,
    )
```
